8 devices in a mesh: dp: 1 (over z), tp: 8 (over y, x, core).
Axes of the slice: x: 2, y: 2, z: 1, core: 2. Of those that a mesh axis runs over, the one named last changes fastest.
Arguments:
- out_y1: float32 [32, 96, 4096], P('dp')
- out_y2: float32 [32, 96, 4096], P('dp')
- cot_y1: float32 [32, 96, 4096], P('dp')
- cot_y2: float32 [32, 96, 4096], P('dp')
- w_qkv: bfloat16 [1, 4096, 32, 3, 128], P(None, None, 'tp')
- w_out: bfloat16 [1, 32, 128, 4096], P(None, 'tp')
- w_up: bfloat16 [1, 4096, 16384], P(None, None, 'tp')
- w_down: bfloat16 [1, 16384, 4096], P(None, 'tp')
Outputs:
- output 1: float32 [32, 96, 4096], P('dp')
- output 2: float32 [32, 96, 4096], P('dp')
- output 3: float32 [32, 96, 4096], P('dp')
- output 4: float32 [32, 96, 4096], P('dp')
- output 5: float32 [1, 4096, 32, 3, 128], P('dp', None, 'tp')
- output 6: float32 [1, 32, 128, 4096], P('dp', 'tp')
- output 7: float32 [1, 4096, 16384], P('dp', None, 'tp')
- output 8: float32 [1, 16384, 4096], P('dp', 'tp')
All inputs are finite; a program needn't handle non-finite values.
Results may differ from the reference program's by a relative error of at most 0.0131098.
Values are sent between devices in bfloat16 or wider.
A program may use at most 2.25 GiB of HBM per device.

```python
import math
import jax
import jax.numpy as jnp
from jax import lax

D = 4096
HEADS = 32
FF = 16384
SEQ = 96
SEQS_DEV = 4
LAYERS = 1
TP = 8

BATCH = SEQS_DEV * TP
HEAD = D // HEADS
TOKENS = BATCH * SEQ
SCORE_SCALE = 1.0 / math.sqrt(HEAD)
NORM_EPS = 1e-6


def setup_inputs(seed: int = 0, part: int = 0) -> dict:
    weight_keys = jax.random.split(jax.random.key(seed), 4)
    act_keys = jax.random.split(jax.random.fold_in(jax.random.key(seed + 1), part), 4)
    act_shape = (BATCH, SEQ, D)
    in_scale = 1.0 / math.sqrt(D)
    hid_scale = 1.0 / math.sqrt(FF)
    attn_gain = max(1.0, math.sqrt(SEQ / 55.0))
    qkv_gain = jnp.array([1.4142, 1.4142, 1.0], jnp.float32).reshape(1, 1, 1, 3, 1)
    w_qkv = jax.random.normal(weight_keys[0], (LAYERS, D, HEADS, 3, HEAD), jnp.float32) * qkv_gain * in_scale
    w_out = jax.random.normal(weight_keys[1], (LAYERS, HEADS, HEAD, D), jnp.float32) * (0.4 * attn_gain * in_scale)
    w_up = jax.random.normal(weight_keys[2], (LAYERS, D, FF), jnp.float32) * in_scale
    w_down = jax.random.normal(weight_keys[3], (LAYERS, FF, D), jnp.float32) * (0.6 * hid_scale)
    return {
        "out_y1": jax.random.normal(act_keys[0], act_shape, jnp.float32),
        "out_y2": jax.random.normal(act_keys[1], act_shape, jnp.float32),
        "cot_y1": jax.random.normal(act_keys[2], act_shape, jnp.float32),
        "cot_y2": jax.random.normal(act_keys[3], act_shape, jnp.float32),
        "w_qkv": w_qkv.astype(jnp.bfloat16),
        "w_out": w_out.astype(jnp.bfloat16),
        "w_up": w_up.astype(jnp.bfloat16),
        "w_down": w_down.astype(jnp.bfloat16),
    }


def rms_fwd(x_in):
    inv_rms = lax.rsqrt(jnp.mean(x_in * x_in, axis=-1, keepdims=True) + NORM_EPS)
    return inv_rms, x_in * inv_rms


def rms_back(inv_rms, normed, grad_n):
    return inv_rms * (grad_n - normed * jnp.mean(normed * grad_n, axis=-1, keepdims=True))


def mlp_block(x_in, cot_out, w_up, w_down):
    inv_rms, normed = rms_fwd(x_in)
    n_bf = normed.astype(jnp.bfloat16)
    hidden = jnp.dot(n_bf, w_up, preferred_element_type=jnp.float32)
    act_f, gelu_back = jax.vjp(jax.nn.gelu, hidden)
    act_bf = act_f.astype(jnp.bfloat16)
    branch = jnp.dot(act_bf, w_down, preferred_element_type=jnp.float32)
    cot_bf = cot_out.astype(jnp.bfloat16)
    g_down = jnp.dot(act_bf.T, cot_bf, preferred_element_type=jnp.float32)
    grad_act = jnp.dot(cot_bf, w_down.T, preferred_element_type=jnp.float32)
    grad_hid = gelu_back(grad_act)[0].astype(jnp.bfloat16)
    g_up = jnp.dot(n_bf.T, grad_hid, preferred_element_type=jnp.float32)
    grad_n = jnp.dot(grad_hid, w_up.T, preferred_element_type=jnp.float32)
    return branch, rms_back(inv_rms, normed, grad_n), g_up, g_down


def attn_probs(qkv_seq):
    q_rows = qkv_seq[:, :, 0].astype(jnp.float32)
    k_rows = qkv_seq[:, :, 1].astype(jnp.float32)
    scores = jnp.einsum("qhe,khe->hqk", q_rows, k_rows) * SCORE_SCALE
    return jax.nn.softmax(scores, axis=-1)


def attn_seq_fwd(qkv_seq):
    prob_f = attn_probs(qkv_seq).astype(jnp.bfloat16).astype(jnp.float32)
    v_rows = qkv_seq[:, :, 2].astype(jnp.float32)
    return jnp.einsum("hqk,khe->qhe", prob_f, v_rows).astype(jnp.bfloat16)


def attn_seq_back(seq_args):
    qkv_seq, grad_o = seq_args
    attn_prob = attn_probs(qkv_seq)
    prob_f = attn_prob.astype(jnp.bfloat16).astype(jnp.float32)
    q_rows = qkv_seq[:, :, 0].astype(jnp.float32)
    k_rows = qkv_seq[:, :, 1].astype(jnp.float32)
    v_rows = qkv_seq[:, :, 2].astype(jnp.float32)
    grad_of = grad_o.astype(jnp.float32)
    grad_p = jnp.einsum("qhe,khe->hqk", grad_of, v_rows)
    grad_v = jnp.einsum("hqk,qhe->khe", prob_f, grad_of)
    grad_s = attn_prob * (grad_p - jnp.sum(grad_p * attn_prob, axis=-1, keepdims=True)) * SCORE_SCALE
    grad_s = grad_s.astype(jnp.bfloat16).astype(jnp.float32)
    grad_q = jnp.einsum("hqk,khe->qhe", grad_s, k_rows)
    grad_k = jnp.einsum("hqk,qhe->khe", grad_s, q_rows)
    return jnp.stack([grad_q, grad_k, grad_v], axis=2).astype(jnp.bfloat16)


def attn_block(x_in, cot_out, w_qkv, w_out):
    inv_rms, normed = rms_fwd(x_in)
    n_bf = normed.astype(jnp.bfloat16)
    qkv_mat = w_qkv.reshape(D, 3 * D)
    out_mat = w_out.reshape(D, D)
    qkv = jnp.dot(n_bf, qkv_mat, preferred_element_type=jnp.float32).astype(jnp.bfloat16)
    qkv = qkv.reshape(BATCH, SEQ, HEADS, 3, HEAD)
    attn_out = lax.map(attn_seq_fwd, qkv).reshape(TOKENS, D)
    branch = jnp.dot(attn_out, out_mat, preferred_element_type=jnp.float32)
    cot_bf = cot_out.astype(jnp.bfloat16)
    g_out = jnp.dot(attn_out.T, cot_bf, preferred_element_type=jnp.float32).reshape(HEADS, HEAD, D)
    grad_o = jnp.dot(cot_bf, out_mat.T, preferred_element_type=jnp.float32).astype(jnp.bfloat16)
    grad_o = grad_o.reshape(BATCH, SEQ, HEADS, HEAD)
    grad_qkv = lax.map(attn_seq_back, (qkv, grad_o)).reshape(TOKENS, 3 * D)
    g_qkv = jnp.dot(n_bf.T, grad_qkv, preferred_element_type=jnp.float32).reshape(D, HEADS, 3, HEAD)
    grad_n = jnp.dot(grad_qkv, qkv_mat.T, preferred_element_type=jnp.float32)
    return branch, rms_back(inv_rms, normed, grad_n), g_qkv, g_out


def reference(out_y1, out_y2, cot_y1, cot_y2, w_qkv, w_out, w_up, w_down):
    def layer_step(carry, weights):
        run_y1, run_y2, run_c1, run_c2 = carry
        layer_qkv, layer_out, layer_up, layer_down = weights
        g_branch, g_grad, g_up, g_down = mlp_block(run_y1, run_c2, layer_up, layer_down)
        low_x2 = run_y2 - g_branch
        run_c1 = run_c1 + g_grad
        f_branch, f_grad, g_qkv, g_out = attn_block(low_x2, run_c1, layer_qkv, layer_out)
        low_x1 = run_y1 - f_branch
        run_c2 = run_c2 + f_grad
        return (low_x1, low_x2, run_c1, run_c2), (g_qkv, g_out, g_up, g_down)

    init = (out_y1.reshape(TOKENS, D), out_y2.reshape(TOKENS, D), cot_y1.reshape(TOKENS, D), cot_y2.reshape(TOKENS, D))
    final, grads = lax.scan(layer_step, init, (w_qkv, w_out, w_up, w_down), reverse=True)
    return (final[0].reshape(BATCH, SEQ, D), final[1].reshape(BATCH, SEQ, D), final[2].reshape(BATCH, SEQ, D), final[3].reshape(BATCH, SEQ, D), grads[0], grads[1], grads[2], grads[3])
```

```python
import functools
import math
import jax
import jax.numpy as jnp
from jax import lax
from jax.experimental import pallas as pl
from jax.sharding import PartitionSpec as P


NORM_EPS = 1e-6
ROW_BLOCK = 128
SEQ_BLOCK = 2
F32 = jnp.float32
BF16 = jnp.bfloat16


def dot(lhs, rhs, lhs_dim, rhs_dim):
    return lax.dot_general(lhs, rhs, (((lhs_dim,), (rhs_dim,)), ((), ())), preferred_element_type=F32)


def rms_kernel(x_ref, n_ref, *copy_ref):
    x_in = x_ref[...]
    inv_rms = lax.rsqrt(jnp.mean(x_in * x_in, axis=-1, keepdims=True) + NORM_EPS)
    n_ref[...] = (x_in * inv_rms).astype(BF16)
    for ref in copy_ref:
        ref[...] = x_in


def rms_rows(x_in, with_copy):
    rows, width = x_in.shape
    spec = pl.BlockSpec((ROW_BLOCK, width), lambda i: (i, 0))
    shapes = [jax.ShapeDtypeStruct(x_in.shape, BF16)] + [jax.ShapeDtypeStruct(x_in.shape, F32)] * with_copy
    return pl.pallas_call(
        rms_kernel,
        grid=(rows // ROW_BLOCK,),
        in_specs=[spec],
        out_specs=[spec] * len(shapes),
        out_shape=shapes,
        cost_estimate=pl.CostEstimate(flops=rows * width * 256, bytes_accessed=rows * width * 6, transcendentals=0),
        name="rms_rows",
    )(x_in)


def rms_back_kernel(x_ref, grad_ref, cot_ref, out_ref, *bf_ref):
    x_in = x_ref[...]
    grad_n = grad_ref[...].astype(F32)
    inv_rms = lax.rsqrt(jnp.mean(x_in * x_in, axis=-1, keepdims=True) + NORM_EPS)
    normed = x_in * inv_rms
    inner = jnp.mean(normed * grad_n, axis=-1, keepdims=True)
    total = cot_ref[...] + inv_rms * (grad_n - normed * inner)
    out_ref[...] = total
    for ref in bf_ref:
        ref[...] = total.astype(BF16)


def rms_back_rows(x_in, grad_n, cot, with_bf16):
    rows, width = x_in.shape
    spec = pl.BlockSpec((ROW_BLOCK, width), lambda i: (i, 0))
    shapes = [jax.ShapeDtypeStruct(x_in.shape, F32)] + [jax.ShapeDtypeStruct(x_in.shape, BF16)] * with_bf16
    return pl.pallas_call(
        rms_back_kernel,
        grid=(rows // ROW_BLOCK,),
        in_specs=[spec] * 3,
        out_specs=[spec] * len(shapes),
        out_shape=shapes,
        cost_estimate=pl.CostEstimate(flops=rows * width * 512, bytes_accessed=rows * width * 16, transcendentals=0),
        name="rms_back_rows",
    )(x_in, grad_n, cot)


def head_probs(qkv_ref, rows, col, head):
    q_rows, k_rows, v_rows = (qkv_ref[rows, pl.ds(col + part * head, head)] for part in range(3))
    scores = dot(q_rows, k_rows, 1, 1) * (1.0 / math.sqrt(head))
    unnorm = jnp.exp(scores - jnp.max(scores, axis=-1, keepdims=True))
    return q_rows, k_rows, v_rows, unnorm / jnp.sum(unnorm, axis=-1, keepdims=True)


def attn_fwd_kernel(seq, head, qkv_ref, out_ref):
    for start in range(0, qkv_ref.shape[0], seq):
        rows = pl.ds(start, seq)
        for idx in range(out_ref.shape[1] // head):
            _, _, v_rows, prob = head_probs(qkv_ref, rows, 3 * head * idx, head)
            out_ref[rows, pl.ds(idx * head, head)] = dot(prob.astype(BF16), v_rows, 1, 0).astype(BF16)


def attn_back_kernel(seq, head, qkv_ref, grad_o_ref, grad_ref):
    for start in range(0, qkv_ref.shape[0], seq):
        rows = pl.ds(start, seq)
        for idx in range(grad_o_ref.shape[1] // head):
            col = 3 * head * idx
            q_rows, k_rows, v_rows, prob = head_probs(qkv_ref, rows, col, head)
            grad_o = grad_o_ref[rows, pl.ds(idx * head, head)]
            grad_p = dot(grad_o, v_rows, 1, 1)
            inner = jnp.sum(grad_p * prob, axis=-1, keepdims=True)
            grad_s = (prob * (grad_p - inner) * (1.0 / math.sqrt(head))).astype(BF16)
            grads = (dot(grad_s, k_rows, 1, 0), dot(grad_s, q_rows, 0, 0), dot(prob.astype(BF16), grad_o, 0, 0))
            for part, grad in enumerate(grads):
                grad_ref[rows, pl.ds(col + part * head, head)] = grad.astype(BF16)


def attn_call(kernel, seq, head, out_cols, *arrays):
    rows = arrays[0].shape[0]
    block = SEQ_BLOCK * seq
    spec = lambda cols: pl.BlockSpec((block, cols), lambda i: (i, 0))
    return pl.pallas_call(
        functools.partial(kernel, seq, head),
        grid=(rows // block,),
        in_specs=[spec(array.shape[1]) for array in arrays],
        out_specs=spec(out_cols),
        out_shape=jax.ShapeDtypeStruct((rows, out_cols), BF16),
        cost_estimate=pl.CostEstimate(flops=rows * 3072 * 2048, bytes_accessed=rows * 4096, transcendentals=0),
    )(*arrays)


def solution(mesh):
    n_tp = mesh.shape["tp"]
    act_spec = P("dp", None, None)
    weight_specs = (P(None, None, "tp", None, None), P(None, "tp", None, None), P(None, None, "tp"), P(None, "tp", None))
    grad_specs = (P("dp", None, "tp", None, None), P("dp", "tp", None, None), P("dp", None, "tp"), P("dp", "tp", None))
    partner = [(i, i ^ 1) for i in range(n_tp)]
    chips = [[i for i in range(n_tp) if i % 2 == core] for core in range(2)]

    def halves(rows_in):
        core = lax.rem(lax.axis_index("tp"), 2)
        blocks = rows_in.reshape(n_tp // 2, 2, rows_in.shape[0] // n_tp, rows_in.shape[1])
        pick = lambda which: lax.dynamic_index_in_dim(blocks, which, 1, keepdims=False).reshape(-1, rows_in.shape[1])
        return pick(core), pick(1 - core)

    def scatter_product(lhs, rhs, rhs_dim, travel, fill, behind=(), after=()):
        keep, send = halves(lhs)
        send, after = lax.optimization_barrier((send, after))
        got = lax.ppermute(dot(send, rhs, 1, rhs_dim).astype(travel), "tp", partner)
        keep, fill = lax.optimization_barrier((keep, fill))
        chip_sum = (dot(keep, rhs, 1, rhs_dim) + got.astype(F32)).astype(travel)
        chip_sum, fill, behind = lax.optimization_barrier((chip_sum, fill, behind))
        own = lax.psum_scatter(chip_sum, "tp", scatter_dimension=0, tiled=True, axis_index_groups=chips)
        return own, fill, behind, after

    def gather(shard):
        return lax.all_gather(shard, "tp", axis=0, tiled=True)

    def layer(run_y1, run_y2, run_c1, run_c2, w_qkv, w_out, w_up, w_down, seqs):
        rows, width = run_y1.shape
        heads, head = w_qkv.shape[1], w_qkv.shape[3]
        wq_mat = w_qkv.reshape(width, heads * 3 * head)
        wo_mat = w_out.reshape(heads * head, width)
        wo_all = gather(wo_mat).reshape(n_tp, heads * head, width)

        (n1,) = rms_rows(run_y1, False)
        hidden = dot(n1, w_up, 1, 0)
        act_f, gelu_back = jax.vjp(jax.nn.gelu, hidden)
        act_bf = act_f.astype(BF16)
        c2_bf = run_c2.astype(BF16)
        g_own, c2_bf, wo_all, _ = scatter_product(act_bf, w_down, 0, F32, c2_bf, wo_all)
        own_at = lax.axis_index("tp") * (rows // n_tp)
        x2_own = lax.dynamic_slice_in_dim(run_y2, own_at, rows // n_tp, 0) - g_own

        grad_hid = gelu_back(dot(c2_bf, w_down, 1, 1))[0].astype(BF16)
        gn_own = scatter_product(grad_hid, w_up, 1, BF16, ())[0]
        x2 = gather(x2_own)
        gn = gather(gn_own)
        g_down = dot(act_bf, c2_bf, 0, 0)
        g_up = dot(n1, grad_hid, 0, 0)

        x2, g_down, g_up = lax.optimization_barrier((x2, g_down, g_up))
        n2, x2_out = rms_rows(x2, True)
        qkv = dot(n2, wq_mat, 1, 0).astype(BF16)
        attn_out = attn_call(attn_fwd_kernel, rows // seqs, head, heads * head, qkv)
        attn_out, gn = lax.optimization_barrier((attn_out, gn))
        c1, c1_bf = rms_back_rows(run_y1, gn, run_c1, True)
        o_all = lax.all_gather(attn_out, "tp", axis=0)
        g_out = dot(attn_out, c1_bf, 0, 0).reshape(w_out.shape)

        grad_o = dot(c1_bf, wo_mat, 1, 1).astype(BF16)
        grad_qkv = attn_call(attn_back_kernel, rows // seqs, head, heads * 3 * head, qkv, grad_o)
        fn_own, g_out, _, o_all = scatter_product(grad_qkv, wq_mat, 1, BF16, g_out, (), o_all)
        x1 = run_y1 - jnp.einsum("jtk,jkd->td", o_all, wo_all, preferred_element_type=F32)
        fn_own, x1 = lax.optimization_barrier((fn_own, x1))
        fn = gather(fn_own)
        g_qkv = dot(n2, grad_qkv, 0, 0).reshape(w_qkv.shape)
        (c2,) = rms_back_rows(x2, fn, run_c2, False)
        return x1, x2_out, c1, c2, g_qkv, g_out, g_up, g_down

    def local_backward(out_y1, out_y2, cot_y1, cot_y2, w_qkv, w_out, w_up, w_down):
        seqs, width = out_y1.shape[0], out_y1.shape[2]
        state = tuple(array.reshape(-1, width) for array in (out_y1, out_y2, cot_y1, cot_y2))
        per_layer = []
        for idx in reversed(range(w_qkv.shape[0])):
            result = layer(*state, w_qkv[idx], w_out[idx], w_up[idx], w_down[idx], seqs)
            state = result[:4]
            per_layer.insert(0, result[4:])
        stacked = tuple(jnp.stack(slot) for slot in zip(*per_layer))
        return tuple(array.reshape(out_y1.shape) for array in state) + stacked

    return jax.shard_map(local_backward, mesh=mesh, in_specs=(act_spec,) * 4 + weight_specs, out_specs=(act_spec,) * 4 + grad_specs, check_vma=False)
```

```python
import functools
import math
import jax
import jax.numpy as jnp
from jax import lax
from jax.experimental import pallas as pl
from jax.experimental.layout import Layout, with_layout_constraint
from jax.sharding import PartitionSpec as P


NORM_EPS = 1e-6
ROW_BLOCK = 128
SEQ_BLOCK = 2
PARTS = 2
F32 = jnp.float32
BF16 = jnp.bfloat16


def dot(lhs, rhs, lhs_dim, rhs_dim):
    return lax.dot_general(lhs, rhs, (((lhs_dim,), (rhs_dim,)), ((), ())), preferred_element_type=F32)


def row_call(kernel, rows, base, arrays, outs, flops, carried=()):
    width = arrays[0].shape[1]
    first = base // ROW_BLOCK
    spec = lambda tall: pl.BlockSpec((ROW_BLOCK, width), lambda i: (i + first if tall else i, 0))
    n_in, n_out = len(arrays), len(outs)

    def body(*refs):
        kernel(*refs[:n_in], *refs[n_in + len(carried):])

    return pl.pallas_call(
        body,
        grid=(rows // ROW_BLOCK,),
        in_specs=[spec(array.shape[0] > rows) for array in arrays] + [pl.BlockSpec(memory_space=pl.ANY)] * len(carried),
        out_specs=[spec(out.shape[0] > rows) for out in outs],
        out_shape=outs,
        input_output_aliases={n_in + i: n_out - len(carried) + i for i in range(len(carried))},
        cost_estimate=pl.CostEstimate(flops=rows * width * flops, bytes_accessed=rows * width * 12, transcendentals=0),
    )(*arrays, *carried)


def rms_kernel(x_ref, n_ref, *copy_ref):
    x_in = x_ref[...]
    inv_rms = lax.rsqrt(jnp.mean(x_in * x_in, axis=-1, keepdims=True) + NORM_EPS)
    n_ref[...] = (x_in * inv_rms).astype(BF16)
    for ref in copy_ref:
        ref[...] = x_in


def rms_back_kernel(x_ref, grad_ref, cot_ref, *out_refs):
    x_in = x_ref[...]
    grad_n = grad_ref[...].astype(F32)
    inv_rms = lax.rsqrt(jnp.mean(x_in * x_in, axis=-1, keepdims=True) + NORM_EPS)
    normed = x_in * inv_rms
    inner = jnp.mean(normed * grad_n, axis=-1, keepdims=True)
    total = cot_ref[...] + inv_rms * (grad_n - normed * inner)
    for ref in out_refs:
        ref[...] = total.astype(ref.dtype)


def head_probs(qkv_ref, rows, col, head):
    q_rows, k_rows, v_rows = (qkv_ref[rows, pl.ds(col + part * head, head)] for part in range(3))
    scores = dot(q_rows, k_rows, 1, 1) * (1.0 / math.sqrt(head))
    unnorm = jnp.exp(scores - jnp.max(scores, axis=-1, keepdims=True))
    return q_rows, k_rows, v_rows, unnorm / jnp.sum(unnorm, axis=-1, keepdims=True)


def attn_kernel(seq, head, qkv_ref, grad_o_ref, out_ref, grad_ref):
    for start in range(0, qkv_ref.shape[0], seq):
        rows = pl.ds(start, seq)
        for idx in range(grad_o_ref.shape[1] // head):
            col = 3 * head * idx
            mine = pl.ds(idx * head, head)
            q_rows, k_rows, v_rows, prob = head_probs(qkv_ref, rows, col, head)
            prob_bf = prob.astype(BF16)
            out_ref[rows, mine] = dot(prob_bf, v_rows, 1, 0).astype(BF16)
            grad_o = grad_o_ref[rows, mine]
            grad_p = dot(grad_o, v_rows, 1, 1)
            inner = jnp.sum(grad_p * prob, axis=-1, keepdims=True)
            grad_s = (prob * (grad_p - inner) * (1.0 / math.sqrt(head))).astype(BF16)
            grads = (dot(grad_s, k_rows, 1, 0), dot(grad_s, q_rows, 0, 0), dot(prob_bf, grad_o, 0, 0))
            for part, grad in enumerate(grads):
                grad_ref[rows, pl.ds(col + part * head, head)] = grad.astype(BF16)


def attn_call(seq, head, base, qkv, grad_o):
    rows, cols = qkv.shape
    block = SEQ_BLOCK * seq
    spec = lambda width, first: pl.BlockSpec((block, width), lambda i: (i + first, 0))
    return pl.pallas_call(
        functools.partial(attn_kernel, seq, head),
        grid=(rows // block,),
        in_specs=[spec(cols, 0), spec(grad_o.shape[1], base // block)],
        out_specs=[spec(grad_o.shape[1], 0), spec(cols, 0)],
        out_shape=[jax.ShapeDtypeStruct((rows, grad_o.shape[1]), BF16), jax.ShapeDtypeStruct((rows, cols), BF16)],
        cost_estimate=pl.CostEstimate(flops=rows * 3072 * 4096, bytes_accessed=rows * 8192, transcendentals=0),
        name="attn",
    )(qkv, grad_o)


def solution(mesh):
    n_tp = mesh.shape["tp"]
    act_spec = P("dp", None, None)
    weight_specs = (P(None, None, "tp", None, None), P(None, "tp", None, None), P(None, None, "tp"), P(None, "tp", None))
    grad_specs = (P("dp", None, "tp", None, None), P("dp", "tp", None, None), P("dp", None, "tp"), P("dp", "tp", None))
    partner = [(i, i ^ 1) for i in range(n_tp)]
    chips = [[i for i in range(n_tp) if i % 2 == core] for core in range(2)]

    def halves(rows_in, parts):
        core = lax.rem(lax.axis_index("tp"), 2)
        blocks = rows_in.reshape(parts, n_tp // 2, 2, -1, rows_in.shape[1])
        pick = lambda which: lax.dynamic_index_in_dim(blocks, which, 2, keepdims=False).swapaxes(0, 1)
        return tuple(pick(which).reshape(-1, rows_in.shape[1]) for which in (core, 1 - core))

    def scatter_product(lhs, rhs, rhs_dim, travel, parts=1, fill=(), behind=(), after=()):
        keep, send = halves(lhs, parts)
        send, after = lax.optimization_barrier((send, after))
        got = lax.ppermute(dot(send, rhs, 1, rhs_dim).astype(travel), "tp", partner)
        keep, fill = lax.optimization_barrier((keep, fill))
        chip_sum = (dot(keep, rhs, 1, rhs_dim) + got.astype(F32)).astype(travel)
        chip_sum, fill, behind = lax.optimization_barrier((chip_sum, fill, behind))
        own = lax.psum_scatter(chip_sum, "tp", scatter_dimension=0, tiled=True, axis_index_groups=chips)
        return own, fill, behind, after

    def gather(shard):
        return lax.all_gather(shard, "tp", axis=0, tiled=True)

    def layer(run_y1, run_y2, run_c1, run_c2, w_qkv, w_out, w_up, w_down, seqs):
        rows, width = run_y1.shape
        seq = rows // seqs
        heads, head = w_qkv.shape[1], w_qkv.shape[3]
        part_rows = rows // PARTS
        share = part_rows // n_tp
        full = lambda dtype: jax.ShapeDtypeStruct((rows, width), dtype)
        wq_mat = w_qkv.reshape(width, heads * 3 * head)
        wo_mat = w_out.reshape(heads * head, width)
        wo_all = gather(wo_mat).reshape(n_tp, heads * head, width)

        (n1,) = row_call(rms_kernel, rows, 0, (run_y1,), (full(BF16),), 256)
        hidden = dot(n1, w_up, 1, 0)
        act_f, gelu_back = jax.vjp(jax.nn.gelu, hidden)
        act_bf = act_f.astype(BF16)
        c2_bf = run_c2.astype(BF16)
        g_own, c2_bf, wo_all, _ = scatter_product(act_bf, w_down, 0, F32, PARTS, c2_bf, wo_all)
        y2_own = lax.dynamic_index_in_dim(run_y2.reshape(PARTS, n_tp, share, width), lax.axis_index("tp"), 1, keepdims=False)

        grad_hid = gelu_back(dot(c2_bf, w_down, 1, 1))[0].astype(BF16)
        gn_own = scatter_product(grad_hid, w_up, 1, BF16)[0]
        gn = gather(gn_own)
        x2 = [gather(y2_own[part] - g_own[part * share:(part + 1) * share]) for part in range(PARTS)]
        g_down = dot(act_bf, c2_bf, 0, 0)
        g_up = with_layout_constraint(dot(n1, grad_hid, 0, 0), Layout((0, 1)))
        gn, g_down, g_up = lax.optimization_barrier((gn, g_down, g_up))

        c1, c1_bf = row_call(rms_back_kernel, rows, 0, (run_y1, gn, run_c1), (full(F32), full(BF16)), 512)
        grad_o = dot(c1_bf, wo_mat, 1, 1).astype(BF16)

        outs, g_qkv, fn_own, x2_out, done = [], 0, [], (), ()
        for part in range(PARTS):
            base = part * part_rows
            part_bf = jax.ShapeDtypeStruct((part_rows, width), BF16)
            n2, copy = row_call(rms_kernel, part_rows, base, (x2[part],), (part_bf, full(F32)), 256, x2_out)
            x2_out = (copy,)
            qkv = dot(n2, wq_mat, 1, 0).astype(BF16)
            qkv, fn_own = lax.optimization_barrier((qkv, fn_own))
            attn_out, grad_qkv = attn_call(seq, head, base, qkv, grad_o)
            outs.append(attn_out)
            g_qkv = g_qkv + dot(n2, grad_qkv, 0, 0)
            if part == PARTS - 1:
                all_out = jnp.concatenate(outs)
                o_all = lax.all_gather(all_out, "tp", axis=0)
                g_out = dot(all_out, c1_bf, 0, 0).reshape(w_out.shape)
                done = (g_out, with_layout_constraint(g_qkv.reshape(w_qkv.shape), Layout((0, 2, 1, 3))))
            own, done, later, _ = scatter_product(grad_qkv, wq_mat, 1, BF16, 1, done, x2[part + 1:])
            x2[part + 1:] = later
            fn_own.append(own)
        x1 = run_y1 - jnp.einsum("jtk,jkd->td", o_all, wo_all, preferred_element_type=F32)
        fn_own[-1], x1 = lax.optimization_barrier((fn_own[-1], x1))
        fn = [gather(own) for own in fn_own]
        g_out, g_qkv = done
        c2 = ()
        for part in range(PARTS):
            c2 = row_call(rms_back_kernel, part_rows, part * part_rows, (x2[part], fn[part], run_c2), (full(F32),), 512, c2)
        return x1, x2_out[0], c1, c2[0], g_qkv, g_out, g_up, g_down

    def local_backward(out_y1, out_y2, cot_y1, cot_y2, w_qkv, w_out, w_up, w_down):
        seqs, width = out_y1.shape[0], out_y1.shape[2]
        state = tuple(array.reshape(-1, width) for array in (out_y1, out_y2, cot_y1, cot_y2))
        per_layer = []
        for idx in reversed(range(w_qkv.shape[0])):
            result = layer(*state, w_qkv[idx], w_out[idx], w_up[idx], w_down[idx], seqs)
            state = result[:4]
            per_layer.insert(0, result[4:])
        stacked = tuple(jnp.stack(slot) for slot in zip(*per_layer))
        return tuple(array.reshape(out_y1.shape) for array in state) + stacked

    return jax.shard_map(local_backward, mesh=mesh, in_specs=(act_spec,) * 4 + weight_specs, out_specs=(act_spec,) * 4 + grad_specs, check_vma=False)
```
